32 devices in a mesh: row: 8 (over z, y), col: 4 (over x, core).
Axes of the slice: x: 2, y: 2, z: 4, core: 2. Of those that a mesh axis runs over, the one named last changes fastest.
Arguments:
- x_blocks: bfloat16 [128, 8, 128, 128], P('row', 'col')
- x_cols: int32 [128, 8], P('row', 'col'), may hold values from 0 to 31, as said below
- x_count: int32 [128, 4], P('row', 'col'), may hold values from 0 to 2, as said below
- y_cols: int32 [128, 48], P('row', 'col'), may hold values from 0 to 31, as said below
- y_count: int32 [128, 4], P('row', 'col'), may hold values from 0 to 12, as said below
- branch_flag: int32 [128], P('row'), may hold values from 0 to 1
Outputs:
- new_blocks: bfloat16 [128, 48, 128, 128], P('row', 'col')
- new_trace: float32 [1], replicated
The draws below stay inside these ranges and needn't reach their ends.
Inputs may be any that keep to these rules, and one draw needn't show every extreme that they name: `x_cols`: within one block row and one column group, the first x_count slots name distinct block columns; other slots hold arbitrary valid columns. Slot 0 of block row I in group I // 32 names column I % 32. `x_count`: reaches 2; at least 1 for block row I in group I // 32. `y_cols`: within one block row and one column group, the first y_count slots name distinct block columns. Slot 0 of block row I in group I // 32 names column I % 32. `y_count`: reaches 12; at least 1 for block row I in group I // 32.
All inputs are finite; a program needn't handle non-finite values.
Results may differ from the reference program's by a relative error of at most 0.0004.
Values may be sent and summed in bfloat16 or wider, within the bound.
No kernel may reach another device: no remote copies, remote signals or barrier semaphores. Data moves between devices by JAX's collectives and lax.ppermute only.
A program may use at most 128 MiB of HBM per device.

```python
import jax
import jax.numpy as jnp
from jax import lax

NB = 128
BS = 128
ROWCAP = 2
YCAP = 12
N_ROW = 8
N_COL = 4


def column_lists(key, slot_count):
    width = NB // N_COL
    scores = jax.random.randint(key, (NB, N_COL, width), 0, 2 ** 20) * width + jnp.arange(width, dtype=jnp.int32)
    rows = jnp.arange(NB, dtype=jnp.int32)
    own_group = (rows // width)[:, None, None] == jnp.arange(N_COL, dtype=jnp.int32)[None, :, None]
    own_col = (rows % width)[:, None, None] == jnp.arange(width, dtype=jnp.int32)[None, None, :]
    scores = jnp.where(own_group & own_col, -1, scores)
    order = jnp.argsort(scores, axis=-1, stable=True).astype(jnp.int32)
    return order[:, :, :slot_count].reshape((NB, N_COL * slot_count))


def diagonal_groups():
    width = NB // N_COL
    rows = jnp.arange(NB, dtype=jnp.int32)
    return (rows // width)[:, None] == jnp.arange(N_COL, dtype=jnp.int32)[None, :]


def draw_x_cols(key, part):
    return column_lists(jax.random.fold_in(key, 11), ROWCAP)


def draw_y_cols(key, part):
    return column_lists(jax.random.fold_in(key, 23), YCAP)


def draw_x_count(key, part):
    values = jax.random.randint(jax.random.fold_in(key, 37), (NB, N_COL), 0, ROWCAP + 2)
    values = jnp.minimum(values, ROWCAP)
    return jnp.where(diagonal_groups(), jnp.maximum(values, 1), values).astype(jnp.int32)


def draw_y_count(key, part):
    values = jax.random.randint(jax.random.fold_in(key, 41), (NB, N_COL), 0, YCAP + 2)
    values = jnp.minimum(values, YCAP)
    return jnp.where(diagonal_groups(), jnp.maximum(values, 1), values).astype(jnp.int32)


def draw_x_blocks(key, part):
    width = NB // N_COL
    shape = (NB, N_COL * ROWCAP, BS, BS)
    base = 0.3 * jax.random.normal(jax.random.fold_in(key, 51), shape, jnp.float32)
    noise = 0.3 * jax.random.normal(jax.random.fold_in(key, 53), (NB, BS, BS), jnp.float32)
    symmetric = (noise + jnp.swapaxes(noise, 1, 2)) * 0.7071
    diag_block = 0.5 * jnp.eye(BS, dtype=jnp.float32)[None] + symmetric
    rows = jnp.arange(NB, dtype=jnp.int32)
    slot_ids = jnp.arange(N_COL * ROWCAP, dtype=jnp.int32)
    is_diag = slot_ids[None, :] == (rows // width * ROWCAP)[:, None]
    mixed = jnp.where(is_diag[:, :, None, None], diag_block[:, None], base)
    return mixed.astype(jnp.bfloat16)


def touch_ends(result, stream_key, least, top_value):
    dims = result.shape
    place = [jax.random.randint(jax.random.fold_in(stream_key, axis), (), 0, dims[axis]) for axis in range(len(dims))]
    result = result.at[tuple(place)].set(least)
    longest = dims.index(max(dims))
    place[longest] = (place[longest] + 1) % dims[longest]
    return result.at[tuple(place)].set(top_value)


def setup_inputs(seed: int = 0) -> dict:
    splits = jax.random.split(jax.random.key(seed), 7)
    return {
        "x_blocks": draw_x_blocks(jax.random.fold_in(splits[6], 71), 0),
        "x_cols": draw_x_cols(jax.random.fold_in(splits[6], 71), 0),
        "x_count": draw_x_count(jax.random.fold_in(splits[6], 71), 0),
        "y_cols": draw_y_cols(jax.random.fold_in(splits[6], 71), 0),
        "y_count": draw_y_count(jax.random.fold_in(splits[6], 71), 0),
        "branch_flag": touch_ends(jax.random.randint(splits[5], (NB,), 0, 2), jax.random.fold_in(splits[5], 1), 0, 1).astype(jnp.int32),
    }


def reference(x_blocks, x_cols, x_count, y_cols, y_count, branch_flag):
    row_width = NB // N_ROW
    col_width = NB // N_COL
    pairs = N_COL * ROWCAP

    def window(index):
        row_group = index // N_COL
        col_group = index % N_COL
        row_start = row_group * row_width
        col_start = col_group * col_width
        row_blocks = lax.dynamic_slice_in_dim(x_blocks, row_start, row_width, 0)
        row_cols = lax.dynamic_slice_in_dim(x_cols, row_start, row_width, 0)
        row_count = lax.dynamic_slice_in_dim(x_count, row_start, row_width, 0)
        row_flags = lax.dynamic_slice_in_dim(branch_flag, row_start, row_width, 0)
        panel_blocks = lax.dynamic_slice_in_dim(x_blocks, col_group * ROWCAP, ROWCAP, 1)
        panel_cols = lax.dynamic_slice_in_dim(x_cols, col_group * ROWCAP, ROWCAP, 1)
        panel_count = lax.dynamic_slice_in_dim(x_count, col_group, 1, 1)[:, 0]
        own_blocks = lax.dynamic_slice_in_dim(row_blocks, col_group * ROWCAP, ROWCAP, 1)
        own_cols = lax.dynamic_slice_in_dim(row_cols, col_group * ROWCAP, ROWCAP, 1)
        own_count = lax.dynamic_slice_in_dim(row_count, col_group, 1, 1)
        win_rows = lax.dynamic_slice_in_dim(y_cols, row_start, row_width, 0)
        win_cols = lax.dynamic_slice_in_dim(win_rows, col_group * YCAP, YCAP, 1)
        count_rows = lax.dynamic_slice_in_dim(y_count, row_start, row_width, 0)
        win_count = lax.dynamic_slice_in_dim(count_rows, col_group, 1, 1)

        pair_ids = jnp.arange(pairs, dtype=jnp.int32)
        groups = pair_ids // ROWCAP
        inner_rows = (groups[None, :] * col_width + row_cols).astype(jnp.int32)
        live = (pair_ids % ROWCAP)[None, :] < jnp.take(row_count, groups, axis=1)
        inner_blocks = panel_blocks[inner_rows]
        inner_cols = panel_cols[inner_rows]
        inner_count = panel_count[inner_rows]
        slot_ids = jnp.arange(ROWCAP, dtype=jnp.int32)
        inner_live = slot_ids[None, None, :] < inner_count[..., None]
        partial_value = jnp.einsum("ipab,ipsbc->ipsac", row_blocks.astype(jnp.float32), inner_blocks.astype(jnp.float32))
        y_live = jnp.arange(YCAP, dtype=jnp.int32)[None, :] < win_count
        route = (inner_cols[:, None, :, :] == win_cols[:, :, None, None]) & inner_live[:, None, :, :]
        route = route & live[:, None, :, None] & y_live[:, :, None, None]
        product = jnp.einsum("iyps,ipsac->iyac", route.astype(jnp.float32), partial_value)

        own_ids = jnp.arange(ROWCAP, dtype=jnp.int32)
        own_match = (own_cols[:, None, :] == win_cols[:, :, None]) & (own_ids[None, None, :] < own_count[:, :, None])
        own_term = jnp.einsum("iyq,iqab->iyab", own_match.astype(jnp.float32), own_blocks.astype(jnp.float32))
        flip = (row_flags == 1)[:, None, None, None]
        updated = jnp.where(flip, 2.0 * own_term - product, product)
        updated = jnp.where(y_live[..., None, None], updated, jnp.zeros((), updated.dtype))
        rows_global = row_start + jnp.arange(row_width, dtype=jnp.int32)[:, None]
        diagonal = (rows_global == col_start + win_cols) & y_live
        traces = jnp.trace(updated, axis1=2, axis2=3)
        trace_part = jnp.sum(jnp.where(diagonal, traces, jnp.zeros((), traces.dtype)))
        return updated.astype(jnp.bfloat16), trace_part

    indices = jnp.arange(N_ROW * N_COL, dtype=jnp.int32)
    updated, traces = lax.map(window, indices)
    updated = updated.reshape((N_ROW, N_COL, row_width, YCAP, BS, BS))
    updated = updated.transpose((0, 2, 1, 3, 4, 5)).reshape((NB, N_COL * YCAP, BS, BS))
    return updated, jnp.sum(traces).reshape((1,))
```

```python
import functools

import jax
import jax.numpy as jnp
from jax import lax
from jax.experimental import pallas as pl
from jax.experimental.pallas import tpu as pltpu
from jax.sharding import PartitionSpec as P


LIST_CAP = 14

F32 = jnp.float32
BF16 = jnp.bfloat16
I32 = jnp.int32


def iota(shape, axis):
    return lax.broadcasted_iota(I32, shape, axis)


def plan_kernel(geo, meta_refs, own_ref, place_ref, sends_ref, rows_ref, flag_ref):
    zs, ys, height, cols, cap, ycap, width = geo
    near = ys * height
    total = zs * near
    pairs = cols * cap
    row_index = place_ref[0]
    col_index = place_ref[1]
    z0 = row_index // ys
    y0 = lax.rem(row_index, ys)

    def global_row(rel):
        oz = rel // near
        rest = lax.rem(rel, near)
        oy = rest // height
        z = lax.rem(z0 + oz, zs)
        y = lax.rem(y0 + oy, ys)
        return (z * ys + y) * height + lax.rem(rest, height)

    lane_rows = global_row(iota((1, total), 1))
    metas = [ref[...] for ref in meta_refs]

    adjacency = jnp.zeros((total, total), F32)
    pair_of = jnp.zeros((height, total), F32)
    for j in range(cols):
        group = lax.rem(col_index + j, cols)
        for s in range(cap):
            target = group * width + metas[j][:, s : s + 1]
            live = metas[j][:, cap : cap + 1] > s
            hit = (lane_rows == target) & live
            adjacency += jnp.where(hit, 1.0, 0.0)
            pair_of += jnp.where(hit[:height], float(j * cap + s), 0.0)

    upper = iota((total, total), 0)
    right = iota((total, total), 1)
    before = jnp.where(upper < right, 1.0, 0.0).astype(BF16)
    same = (upper // near) == (right // near)
    before_in_group = jnp.where((upper < right) & same, 1.0, 0.0).astype(BF16)
    in_group = jnp.where(same, 1.0, 0.0).astype(BF16)

    def mm(a, b):
        return jnp.dot(a.astype(BF16), b, preferred_element_type=F32)

    groups = zs * ys
    group_oz = iota((groups, total), 0) // ys
    lane_oz = iota((groups, total), 1) // near
    worst = jnp.zeros((1, 1), F32)
    for j in range(cols):
        meta = metas[j]
        flat = meta[:, : cap + 1].astype(F32)
        flat = jnp.concatenate([flat, jnp.zeros((total, 128 - cap - 1), F32)], axis=1)
        turned = flat.T
        slot_of = jnp.zeros((total, width), F32)
        wide = iota((total, width), 1)
        for t in range(ycap):
            hit = (wide == meta[:, cap + 1 + t : cap + 2 + t]) & (meta[:, cap + 1 + ycap : cap + 2 + ycap] > t)
            slot_of += jnp.where(hit, float(t + 1), 0.0)
        tall = iota((width, total), 0).astype(F32)
        slots, needs = [], []
        for q in range(cap):
            spread = jnp.where((tall == turned[q : q + 1, :]) & (turned[cap : cap + 1, :] > float(q)), 1.0, 0.0)
            slot = mm(slot_of, spread.astype(BF16))
            match = slot * adjacency
            need = jnp.concatenate(
                [jnp.max(match[g * height : (g + 1) * height], axis=0, keepdims=True) for g in range(groups)], axis=0
            )
            slots.append(slot)
            needs.append(jnp.where(need > 0.0, 1.0, 0.0))
        counts = sum(mm(need, in_group) for need in needs)
        far = jnp.where(group_oz != lane_oz, counts, 0.0)
        worst = jnp.maximum(worst, jnp.max(jnp.max(far, axis=1, keepdims=True), axis=0, keepdims=True))
        if j == 0:
            own_slots, own_needs, own_slot_of = slots, needs, slot_of
    flag_ref[...] = jnp.broadcast_to(jnp.where(worst > float(LIST_CAP), 1, 0).astype(I32), flag_ref.shape)

    positions = []
    earlier = jnp.zeros((groups, total), F32)
    for q in range(cap):
        positions.append(mm(own_needs[q], before_in_group) + earlier)
        earlier = earlier + mm(own_needs[q], in_group)

    depth = sends_ref.shape[0]
    out_lane = iota((depth, 128), 1)
    order = iota((depth, near), 0).astype(F32)
    slot_id = iota((1, near), 1).astype(F32) * float(cap)
    sends = jnp.zeros((depth, 128), F32)
    for d in range(1, zs):
        picked = jnp.zeros((depth, 1), F32)
        for q in range(cap):
            position = positions[q][d * ys : d * ys + 1, :near]
            need = own_needs[q][d * ys : d * ys + 1, :near]
            chosen = (order == position) & (need > 0.0)
            picked += jnp.sum(jnp.where(chosen, slot_id + float(q), 0.0), axis=1, keepdims=True)
        sends += jnp.where(out_lane == d, picked, 0.0)
    sends_ref[...] = sends.astype(I32)

    lane = iota((height, 128), 1)
    lanes = iota((1, total), 1)
    lane_group = lanes // near
    rank_base = jnp.zeros((height, 1), F32)
    listed = [jnp.zeros((height, 128), F32) for _ in range(2)]
    own_lane = iota((height, total), 1) == iota((height, total), 0)
    head = jnp.zeros((height, 128), F32)
    entries = pairs * cap
    for q in range(cap):
        slot = own_slots[q][:height]
        hit = jnp.where(slot * adjacency[:height] > 0.0, 1.0, 0.0)
        rank = mm(hit, before) + rank_base
        rank_base = rank_base + jnp.sum(hit, axis=1, keepdims=True)
        local = (lanes * cap + q).astype(F32)
        remote = ((near * cap) + (lane_group - 1) * LIST_CAP).astype(F32) + positions[q][0:1]
        sparse_at = jnp.where(lane_group == 0, local, remote)
        low = pair_of * float(ycap) + (slot - 1.0)
        for v, place in enumerate((sparse_at, local)):
            code = place * float(pairs * ycap) + low
            for e in range(entries):
                value = jnp.sum(jnp.where((rank == float(e)) & (hit > 0.0), code, 0.0), axis=1, keepdims=True)
                listed[v] += jnp.where(lane == 8 + e, value, 0.0)
        own_term = jnp.sum(jnp.where(own_lane, slot, 0.0), axis=1, keepdims=True)
        head += jnp.where(lane == 3 + q, own_term, 0.0)
    head += jnp.where(lane == 0, rank_base, 0.0)
    head += jnp.where(lane == 1, own_ref[...].astype(F32), 0.0)
    row_ids = global_row(iota((height, width), 0))
    on_diagonal = (row_ids // width == col_index) & (lax.rem(row_ids, width) == iota((height, width), 1))
    diagonal = jnp.sum(jnp.where(on_diagonal, own_slot_of[:height], 0.0), axis=1, keepdims=True)
    head += jnp.where(lane == 2, diagonal, 0.0)
    for v in range(2):
        rows_ref[v] = (head + listed[v]).astype(I32)


def plan(geo, metas, branch_flag, place):
    zs, ys, height, cols, cap, ycap, width = geo
    depth = -(-LIST_CAP // 8) * 8
    return pl.pallas_call(
        lambda *refs: plan_kernel(geo, refs[:cols], *refs[cols:]),
        out_shape=(
            jax.ShapeDtypeStruct((depth, 128), I32),
            jax.ShapeDtypeStruct((2, height, 128), I32),
            jax.ShapeDtypeStruct((8, 128), I32),
        ),
        in_specs=[pl.BlockSpec(memory_space=pltpu.VMEM)] * (cols + 1) + [pl.BlockSpec(memory_space=pltpu.SMEM)],
        out_specs=(pl.BlockSpec(memory_space=pltpu.VMEM),) * 3,
        name="plan",
    )(*metas, branch_flag.reshape(height, 1), place)


def pack_kernel(parts, zs, per_part, *refs):
    sends_ref = refs[0]
    part_refs = refs[1 : 1 + parts]
    out_refs = refs[1 + parts :]
    for d in range(1, zs):

        @pl.loop(0, LIST_CAP)
        def _(j):
            index = sends_ref[j, d]
            for b in range(parts):

                @pl.when(index // per_part == b)
                def _():
                    out_refs[d - 1][j] = part_refs[b][index - b * per_part]


def pack(sends, parts, zs):
    per_part, size = parts[0].shape[0], parts[0].shape[1:]
    return pl.pallas_call(
        functools.partial(pack_kernel, len(parts), zs, per_part),
        out_shape=[jax.ShapeDtypeStruct((LIST_CAP,) + size, BF16)] * (zs - 1),
        in_specs=[pl.BlockSpec(memory_space=pltpu.SMEM)] + [pl.BlockSpec(memory_space=pltpu.VMEM)] * len(parts),
        out_specs=[pl.BlockSpec(memory_space=pltpu.VMEM)] * (zs - 1),
        name="pack",
    )(sends, *parts)


def compute_kernel(cap, ycap, cols, sizes, *refs):
    rows_ref = refs[0]
    row_refs = refs[1 : 1 + cols]
    panel_refs = refs[1 + cols : 1 + cols + len(sizes)]
    out_ref, trace_ref, row_buf, panel_buf, acc, trace_acc, sems = refs[1 + cols + len(sizes) :]
    i = pl.program_id(0)
    height = pl.num_programs(0)
    pairs = cols * cap
    bs = acc.shape[1]

    @pl.when(i == 0)
    def _():
        copies = []
        for j in range(cols):
            copies.append(pltpu.make_async_copy(row_refs[j], row_buf.at[j], sems.at[j]))
        at = 0
        for n, size in enumerate(sizes):
            copies.append(pltpu.make_async_copy(panel_refs[n], panel_buf.at[pl.ds(at, size)], sems.at[cols + n]))
            at += size
        for copy in copies:
            copy.start()
        acc[...] = jnp.zeros_like(acc)
        trace_acc[...] = jnp.zeros_like(trace_acc)
        for copy in copies:
            copy.wait()

    out_ref[...] = jnp.zeros_like(out_ref)
    count = rows_ref[i, 0]
    flip = rows_ref[i, 1] == 1
    sign = jnp.where(flip, -1.0, 1.0)

    @pl.loop(0, count)
    def _(e):
        code = rows_ref[i, 8 + e]
        t = lax.rem(code, ycap)
        rest = code // ycap
        p = lax.rem(rest, pairs)
        at = rest // pairs
        left = row_buf[p // cap, i * cap + lax.rem(p, cap)]
        acc[t] += jnp.dot(left, panel_buf[at], preferred_element_type=F32)

    for q in range(cap):
        own = rows_ref[i, 3 + q]

        @pl.when(flip & (own > 0))
        def _():
            acc[own - 1] -= 2.0 * row_buf[0, i * cap + q].astype(F32)

    diagonal = rows_ref[i, 2]

    @pl.when(diagonal > 0)
    def _():
        value = acc[diagonal - 1] * sign
        trace_acc[...] += jnp.where(iota((bs, bs), 0) == iota((bs, bs), 1), value, 0.0)

    @pl.loop(0, count)
    def _(e):
        t = lax.rem(rows_ref[i, 8 + e], ycap)
        out_ref[0, t] = (acc[t] * sign).astype(BF16)

    for q in range(cap):
        own = rows_ref[i, 3 + q]

        @pl.when(flip & (own > 0))
        def _():
            out_ref[0, own - 1] = (acc[own - 1] * sign).astype(BF16)
            acc[own - 1] = jnp.zeros((bs, bs), F32)

    @pl.loop(0, count)
    def _(e):
        t = lax.rem(rows_ref[i, 8 + e], ycap)
        acc[t] = jnp.zeros((bs, bs), F32)

    @pl.when(i == height - 1)
    def _():
        part = jnp.sum(jnp.sum(trace_acc[...], axis=0, keepdims=True), axis=1, keepdims=True)
        trace_ref[...] = jnp.broadcast_to(part, trace_ref.shape)


def compute(cap, ycap, rows, row_pieces, panel_pieces):
    height = rows.shape[0]
    cols = len(row_pieces)
    bs = row_pieces[0].shape[-1]
    sizes = [piece.shape[0] for piece in panel_pieces]
    hbm = pl.BlockSpec(memory_space=pl.ANY)
    return pl.pallas_call(
        functools.partial(compute_kernel, cap, ycap, cols, sizes),
        grid=(height,),
        out_shape=(
            jax.ShapeDtypeStruct((height, ycap, bs, bs), BF16),
            jax.ShapeDtypeStruct((8, 128), F32),
        ),
        in_specs=[pl.BlockSpec(memory_space=pltpu.SMEM)] + [hbm] * (cols + len(sizes)),
        out_specs=(
            pl.BlockSpec((1, ycap, bs, bs), lambda i: (i, 0, 0, 0)),
            pl.BlockSpec((8, 128), lambda i: (0, 0)),
        ),
        scratch_shapes=[
            pltpu.VMEM((cols, height * cap, bs, bs), BF16),
            pltpu.VMEM((sum(sizes), bs, bs), BF16),
            pltpu.VMEM((ycap, bs, bs), F32),
            pltpu.VMEM((bs, bs), F32),
            pltpu.SemaphoreType.DMA((cols + len(sizes),)),
        ],
        compiler_params=pltpu.CompilerParams(dimension_semantics=("arbitrary",)),
        name="compute",
    )(rows, *row_pieces, *panel_pieces)


def from_row(value, zs, ys, oz, oy):
    pairs = []
    for z in range(zs):
        for y in range(ys):
            pairs.append(((z + oz) % zs * ys + (y + oy) % ys, z * ys + y))
    return lax.ppermute(value, "row", pairs)


def from_col(value, n, o):
    return lax.ppermute(value, "col", [((c + o) % n, c) for c in range(n)])


def sum_all(value, zs, ys, cols):
    def total(value, name, n, stride, size):
        if size & (size - 1):
            parts = [value]
            for o in range(1, size):
                moved = [(d // stride // size * size + (d // stride + o) % size) * stride + d % stride for d in range(n)]
                parts.append(lax.ppermute(value, name, [(s, d) for d, s in enumerate(moved)]))
            return sum(parts)
        step = 1
        while step < size:
            value = value + lax.ppermute(value, name, [(d ^ (step * stride), d) for d in range(n)])
            step *= 2
        return value

    value = total(value, "col", cols, 1, cols)
    value = total(value, "row", zs * ys, 1, ys) if ys & (ys - 1) == 0 else value
    if ys & (ys - 1) == 0 and zs & (zs - 1) == 0:
        return total(value, "row", zs * ys, ys, zs)
    return lax.psum(value, "row")


def on_device(zs, ys, cols, x_blocks, x_cols, x_count, y_cols, y_count, branch_flag):
    height, cap, bs, _ = x_blocks.shape
    ycap = y_cols.shape[1]
    width = zs * ys * height // cols
    geo = (zs, ys, height, cols, cap, ycap, width)
    own = x_blocks.reshape(height * cap, bs, bs)

    meta = jnp.concatenate([x_cols, x_count, y_cols, y_count], axis=1)
    meta = jnp.concatenate([meta] + [from_row(meta, zs, ys, 0, oy) for oy in range(1, ys)], axis=0)
    meta, first = lax.optimization_barrier((meta, own))
    near = [own] + [from_row(first, zs, ys, 0, oy) for oy in range(1, ys)]
    meta = jnp.concatenate([meta] + [from_col(meta, cols, o) for o in range(1, cols)], axis=0)
    meta, second = lax.optimization_barrier((meta, own))
    row_pieces = [own] + [from_col(second, cols, o) for o in range(1, cols)]
    layers = [meta] + [from_row(meta, zs, ys, oz, 0) for oz in range(1, zs)]
    step = ys * height
    metas = [jnp.concatenate([layer[o * step : (o + 1) * step] for layer in layers], axis=0) for o in range(cols)]

    place = jnp.stack([lax.axis_index("row"), lax.axis_index("col")]).astype(I32)
    sends, rows, flag = plan(geo, metas, branch_flag, place)
    packed = pack(sends, near, zs)
    lists = [from_row(packed[zs - oz - 1], zs, ys, oz, 0) for oz in range(1, zs)]

    blocks, trace_part = compute(cap, ycap, rows[0], row_pieces, near + lists)
    total = sum_all(trace_part, zs, ys, cols)

    def dense(state):
        panel = [from_row(own, zs, ys, oz, oy) if oz or oy else own for oz in range(zs) for oy in range(ys)]
        blocks, trace_part = compute(cap, ycap, rows[1], row_pieces, panel)
        return (jnp.zeros((), I32), blocks, sum_all(trace_part, zs, ys, cols))

    _, blocks, total = lax.while_loop(lambda state: state[0] == 1, dense, (flag[0, 0], blocks, total))
    return (blocks, total[0, :1])


def row_shape(mesh):
    count = mesh.shape["row"]
    try:
        depth = [device.coords[2] for device in mesh.devices[:, 0]]
        ys = depth.count(depth[0])
    except (AttributeError, TypeError):
        ys = 2 if count % 2 == 0 else 1
    if count % ys:
        ys = 1
    return count // ys, ys


def solution(mesh):
    zs, ys = row_shape(mesh)
    return jax.shard_map(
        functools.partial(on_device, zs, ys, mesh.shape["col"]),
        mesh=mesh,
        in_specs=(
            P("row", "col", None, None),
            P("row", "col"),
            P("row", "col"),
            P("row", "col"),
            P("row", "col"),
            P("row"),
        ),
        out_specs=(P("row", "col", None, None), P()),
        check_vma=False,
    )
```
